256 devices in a mesh: arm: 2 (over y), snp: 128 (over z, x, core).
Axes of the slice: x: 4, y: 2, z: 16, core: 2. Of those that a mesh axis runs over, the one named last changes fastest.
The devices are a block of a 4x16x16 slice.
Arguments:
- genotypes: int32 [32768, 1024], P(('arm', 'snp')), parts along dimension 0, may hold values from -2147483648 to 2147483647, as said below
- positions: int32 [32768], P(('arm', 'snp')), parts along dimension 0, may hold values from 2001303 to 28673152, as said below
Outputs:
- linkage: float32 [32768, 1664], P(('arm', 'snp')), parts along dimension 0
The draws below stay inside these ranges and needn't reach their ends.
There are 2 independent parts, one for each index of `arm`. The reference program is written for one: setup_inputs(seed, part) draws one part's arguments, and reference() takes and returns one part's arrays. A program takes and returns all parts, laid end to end along the dimension named above; each array names one. Nothing has to cross between parts.
Inputs may be any that keep to these rules, and one draw needn't show every extreme that they name: `genotypes`: each word holds 16 two-bit codes: the call of sample s sits in bits 2 * (s // 1024) and 2 * (s // 1024) + 1 of word s mod 1024; codes 0, 1, 2 count alternate alleles and code 3 marks a missing call. `positions`: strictly increasing; consecutive SNPs lie 1303 or more base pairs apart.
All inputs are finite; a program needn't handle non-finite values.
Results may differ from the reference program's by a relative error of at most 0.0031.
Values may be sent and summed in bfloat16 or wider, within the bound.
A program may use at most 128 MiB of HBM per device.

```python
import jax
import jax.numpy as jnp
from jax import lax

SNP_DEV = 128
SAMPLES = 16384
REACH = 6
BAND_BP = 1000000
WORDS = 1024
SNPS = 16384
GAP_MIN = 1303
N_SNP = 128


def draw_genotypes(key, part):
    keys = jax.random.split(jax.random.fold_in(key, 11), 8)
    thresh = jax.random.randint(keys[0], (SNPS, 1), 50, 950)
    offset = jax.random.randint(keys[1], (), 0, 24)
    block_id = (jnp.arange(SNPS, dtype=jnp.int32) + offset) // 24
    nblocks = SNPS // 24 + 2
    dosage = jnp.zeros((SNPS, SAMPLES), jnp.int32)
    for strand in range(2):
        shared = jax.random.randint(keys[2 + strand], (nblocks, SAMPLES), 0, 1000)
        fresh = jax.random.randint(keys[4 + strand], (SNPS, SAMPLES), 0, 4000)
        latent = jnp.where(fresh < 1000, fresh, shared[block_id])
        dosage = dosage + (latent < thresh).astype(jnp.int32)
    missing = jax.random.randint(keys[6], (SNPS, SAMPLES), 0, 25) == 0
    codes = jnp.where(missing, 3, dosage).astype(jnp.int32)
    grouped = codes.reshape(SNPS, 16, WORDS)
    packed = jnp.zeros((SNPS, WORDS), jnp.int32)
    for lane in range(16):
        packed = packed | jnp.left_shift(grouped[:, lane, :], 2 * lane)
    return packed


def draw_positions(key, part):
    keys = jax.random.split(jax.random.fold_in(key, 23), 1)
    gaps = jax.random.randint(keys[0], (SNPS,), GAP_MIN, GAP_MIN + GAP_MIN // 4 + 1).astype(jnp.int32)
    top_value = 2 * BAND_BP + SNPS * (GAP_MIN + GAP_MIN // 4)
    running = jnp.cumsum(gaps).astype(jnp.int32)
    return (top_value - (running[-1] - running)).astype(jnp.int32)


def setup_inputs(seed: int = 0, part: int = 0) -> dict:
    seeds = jax.random.split(jax.random.key(seed), 3)
    part_keys = jax.random.split(jax.random.fold_in(seeds[2], part), 3)
    genotypes = draw_genotypes(jax.random.fold_in(jax.random.fold_in(seeds[2], part), 71), part)
    positions = draw_positions(jax.random.fold_in(jax.random.fold_in(seeds[2], part), 71), part)
    return dict(genotypes=genotypes, positions=positions)


def standardize(packed):
    shifts = 2 * jnp.arange(16, dtype=jnp.int32)
    codes = jnp.right_shift(packed[:, None, :], shifts[None, :, None]) & 3
    called = codes != 3
    observed = called.astype(jnp.float32)
    dosage = jnp.where(called, codes, 0).astype(jnp.float32)
    tally = lax.optimization_barrier(jnp.sum(observed, axis=(1, 2)))
    allele = (lax.optimization_barrier(jnp.sum(dosage, axis=(1, 2))) + 1.0) / (2.0 * tally + 2.0)
    spread = lax.rsqrt(2.0 * allele * (1.0 - allele))
    scores = observed * (dosage - 2.0 * allele[:, None, None]) * spread[:, None, None]
    return scores.astype(jnp.bfloat16)

def reference(genotypes, positions):
    blocks = genotypes.reshape(N_SNP, SNP_DEV, WORDS)
    scored = lax.map(standardize, blocks)
    scored = lax.optimization_barrier(scored)
    flat = scored.astype(jnp.float32).reshape(SNPS, SAMPLES)
    margin = REACH * SNP_DEV
    padded = jnp.pad(flat, ((margin, margin), (0, 0)))
    pos_pad = jnp.pad(positions, (margin, margin))
    inside = jnp.pad(jnp.ones((SNPS,), jnp.int32), (margin, margin))
    span = (2 * REACH + 1) * SNP_DEV

    def window(index):
        first = (index * SNP_DEV).astype(jnp.int32)
        rows = lax.dynamic_slice_in_dim(flat, first, SNP_DEV, 0)
        columns = lax.dynamic_slice_in_dim(padded, first, span, 0)
        product = jnp.dot(rows, columns.T, precision=lax.Precision.HIGHEST, preferred_element_type=jnp.float32) / SAMPLES
        row_pos = lax.dynamic_slice_in_dim(positions, first, SNP_DEV, 0)
        col_pos = lax.dynamic_slice_in_dim(pos_pad, first, span, 0)
        col_in = lax.dynamic_slice_in_dim(inside, first, span, 0)
        in_band = (jnp.abs(row_pos[:, None] - col_pos[None, :]) <= BAND_BP) & (col_in[None, :] == 1)
        return jnp.where(in_band, product, jnp.zeros_like(product))
    result = lax.map(window, jnp.arange(N_SNP, dtype=jnp.int32))
    return result.reshape(SNPS, span)
```

```python
import functools

import jax
import jax.numpy as jnp
from jax import lax
from jax.experimental import pallas as pl
from jax.experimental.pallas import tpu as pltpu
from jax.sharding import PartitionSpec as P

REACH = 6
BAND_BP = 1000000
COLS = 4
LANES = 128
CODES = 16
RL, LR, ZRL, ZLR, OWN = range(5)
MESH = pl.DeviceIdType.MESH
I16 = jnp.int16
OWNERS = ((1, (0, 3)), (-1, (2, 3)), (2, (0, 1)), (-2, (0, 1)), (3, (2, 3)), (-3, (0, 3)))


def any_of(col, cols):
    hit = col == cols[0]
    for c in cols[1:]:
        hit = hit | (col == c)
    return hit


def lookup(half, bit, v0, v1, v2, zero):
    high = 2 << bit
    low_set = (half & I16(1 << bit)) != I16(0)
    high_set = (half & I16(high if high < 32768 else -32768)) != I16(0)
    return jnp.where(high_set, jnp.where(low_set, zero, v2), jnp.where(low_set, v1, v0))


def values_of(missing, dosage, samples):
    tally = samples - missing.astype(jnp.float32)
    allele = (dosage.astype(jnp.float32) + 1.0) / (2.0 * tally + 2.0)
    spread = lax.rsqrt(2.0 * allele * (1.0 - allele))
    return [(code - 2.0 * allele) * spread for code in (0.0, 1.0, 2.0)]


def kernel(devices, geno, pos, out, buf, xbuf, own_t, panel, acc, part, tab, place_of,
           lane_tab, meta_out, meta_in, mir_out, mir_in,
           load_sem, x_send, fwd_send, fwd2_send, arrive, meta_send, meta_recv, sib_send,
           part_send, part_recv, mir_send, mir_recv):
    rows = pos.shape[1]
    words = geno.shape[1]
    parts = words // (2 * LANES)
    samples = float(words * CODES)
    me = lax.axis_index("snp")
    chips = devices // 2
    core = lax.rem(me, 2)
    chip = me // 2
    col = lax.rem(chip, COLS)
    base = chip - col

    def rel(offset):
        return lax.rem(chip + offset + chips, chips)

    left = base + lax.rem(col + COLS - 1, COLS)
    right = base + lax.rem(col + 1, COLS)
    sibling = me + 1 - 2 * core

    def core_of(c, k):
        return {"snp": c * 2 + k}

    loads = []
    for e in range(2):
        half = core if e == 0 else 1 - core
        for j in range(parts):
            lane = pl.multiple_of((half * parts + j) * LANES, LANES)
            dst = buf.at[OWN, 0, j] if e == 0 else xbuf.at[j]
            loads.append(pltpu.make_async_copy(geno.at[:, pl.ds(lane, LANES)], dst, load_sem.at[e, j]))
            loads[-1].start()

    def own_piece(e, j):
        return buf.at[OWN, 0, j] if e == 0 else xbuf.at[j]

    barrier = pltpu.get_barrier_semaphore()
    partners = [left, right] + [rel(o) for o in (COLS, -COLS, 1, -1, 2, -2, 3, -3)]
    for c in partners:
        for k in range(2):
            pl.semaphore_signal(barrier, inc=1, device_id=core_of(c, k), device_id_type=MESH)
    pl.semaphore_signal(barrier, inc=1, device_id={"snp": sibling}, device_id_type=MESH)
    for copy in loads:
        copy.wait()
    pl.semaphore_wait(barrier, 2 * len(partners) + 1)

    sends_left = col >= 1
    sends_right = (col == 0) | (col == 3)
    uses_rl = col >= 1
    uses_lr = col <= 2
    dz_rl = jnp.where(col == 3, -1, 1)
    dz_lr = jnp.where(col == 0, 1, -1)
    off_rl = jnp.where(col == 3, -2, 1)
    off_lr = jnp.where(col == 0, 3, jnp.where(col == 1, -1, -2))
    off_zrl = off_rl - COLS * dz_rl
    off_zlr = off_lr - COLS * dz_lr

    def offset_of(s):
        return jnp.where(s == RL, off_rl, jnp.where(s == LR, off_lr, jnp.where(s == ZRL, off_zrl, off_zlr)))

    def uses(s):
        return jnp.where((s == RL) | (s == ZRL), col >= 1, col <= 2)

    def hop(src, send_sem, s, e, j, target):
        return pltpu.make_async_remote_copy(
            src_ref=src, dst_ref=buf.at[s, e, j], send_sem=send_sem, recv_sem=arrive.at[s, e, j],
            device_id=target, device_id_type=MESH)

    def x_hop(e, j, way):
        target = core_of(left if way == RL else right, core if e == 0 else 1 - core)
        return hop(own_piece(e, j), x_send.at[way, e, j], way, e, j, target)

    for way, sends in ((RL, sends_left), (LR, sends_right)):
        @pl.when(sends)
        def _(way=way):
            for j in range(parts):
                for e in range(2):
                    x_hop(e, j, way).start()

    def to_sibling(j):
        return hop(xbuf.at[j], sib_send.at[j], OWN, 1, j, {"snp": sibling})

    for j in range(parts):
        to_sibling(j).start()

    missing = jnp.zeros((rows, LANES), jnp.int32)
    dosage = jnp.zeros((rows, LANES), jnp.int32)
    for e in range(2):
        for j in range(parts):
            word = own_piece(e, j)[...]
            low = word & 0x55555555
            high = lax.shift_right_logical(word, 1) & 0x55555555
            gone = lax.population_count(low & high)
            missing = missing + gone
            dosage = dosage + lax.population_count(low) + 2 * lax.population_count(high) - 3 * gone
    counts = []
    for x in (missing, dosage):
        total = jnp.broadcast_to(jnp.sum(x, axis=1, keepdims=True), (rows, LANES))
        counts.append(total.T[0:1])
    meta_out[0:1] = pos[...]
    meta_out[1:2] = counts[0]
    meta_out[2:3] = counts[1]
    meta_out[3:8] = jnp.zeros((5, LANES), jnp.int32)

    def meta_copy(offset, e):
        k = core if e == 0 else 1 - core
        return pltpu.make_async_remote_copy(
            src_ref=meta_out, dst_ref=meta_in.at[3 - offset, e], send_sem=meta_send.at[3 + offset, e],
            recv_sem=meta_recv.at[3 - offset, e],
            device_id={"snp": sibling} if offset == 0 else core_of(rel(offset), k), device_id_type=MESH)

    meta_copy(0, 1).start()
    for offset, cols in OWNERS:
        @pl.when(any_of(col, cols))
        def _(offset=offset):
            for e in range(2):
                meta_copy(offset, e).start()

    def fill_tables(s, e, counts8):
        columns = [jnp.broadcast_to(counts8.T[:, i:i + 1], (rows, LANES)) for i in range(3)]
        place_of[s, e] = columns[0]
        for i, v in enumerate(values_of(columns[1], columns[2], samples)):
            tab[s, e, i] = v.astype(jnp.bfloat16)

    def batch(s, j, first):
        for e in range(2):
            word = buf[s, e, j]
            halves = word.astype(I16), lax.shift_right_logical(word, 16).astype(I16)
            v0, v1, v2 = (tab[s, e, i] for i in range(3))
            zero = jnp.zeros_like(v0)
            for q in range(CODES):
                panel[e * rows:(e + 1) * rows, q * LANES:(q + 1) * LANES] = lookup(
                    halves[q // 8], 2 * (q % 8), v0, v1, v2, zero)
        product = lax.dot_general(panel[...], own_t[j], (((1,), (0,)), ((), ())),
                                  preferred_element_type=jnp.float32)
        for e in range(2):
            for c in range(2):
                tile = product[e * rows:(e + 1) * rows, c * LANES:(c + 1) * LANES]
                acc[s, e, c] = jnp.where(first, tile, acc[s, e, c] + tile)

    pltpu.make_async_remote_copy(
        src_ref=meta_out, dst_ref=meta_in.at[3, 1], send_sem=meta_send.at[3, 1], recv_sem=meta_recv.at[3, 1],
        device_id={"snp": sibling}, device_id_type=MESH).wait_recv()
    for e in range(2):
        counts8 = meta_out[...] if e == 0 else meta_in[3, 1]
        fill_tables(OWN, e, counts8)
        for i, v in enumerate(values_of(counts8[1:2], counts8[2:3], samples)):
            lane_tab[e, i] = jnp.broadcast_to(v, (rows, LANES)).astype(jnp.bfloat16)

    def own_step(j, carry):
        hop(xbuf.at[j], sib_send.at[j], OWN, 1, j, {"snp": sibling}).wait_recv()
        for e in range(2):
            word = buf[OWN, e, j].T
            halves = word.astype(I16), lax.shift_right_logical(word, 16).astype(I16)
            v0, v1, v2 = (lane_tab[e, i] for i in range(3))
            zero = jnp.zeros_like(v0)
            for q in range(CODES):
                own_t[j, q * LANES:(q + 1) * LANES, e * rows:(e + 1) * rows] = lookup(
                    halves[q // 8], 2 * (q % 8), v0, v1, v2, zero)
        batch(OWN, j, j == 0)
        return carry

    lax.fori_loop(0, parts, own_step, 0)

    def part_copy(s, e):
        return pltpu.make_async_remote_copy(
            src_ref=acc.at[s, e, 1], dst_ref=part.at[s, 1 - e], send_sem=part_send.at[s, e],
            recv_sem=part_recv.at[s, 1 - e], device_id={"snp": sibling}, device_id_type=MESH)

    def part_arrived(s, e):
        pltpu.make_async_remote_copy(
            src_ref=acc.at[s, e, 1], dst_ref=part.at[s, e], send_sem=part_send.at[s, e],
            recv_sem=part_recv.at[s, e], device_id={"snp": sibling}, device_id_type=MESH).wait_recv()

    for e in range(2):
        part_copy(OWN, e).start()

    def table_step(s, carry):
        @pl.when(uses(s))
        def _():
            slot = offset_of(s) + 3
            for e in range(2):
                pltpu.make_async_remote_copy(
                    src_ref=meta_out, dst_ref=meta_in.at[slot, e], send_sem=meta_send.at[slot, e],
                    recv_sem=meta_recv.at[slot, e], device_id={"snp": sibling},
                    device_id_type=MESH).wait_recv()
                fill_tables(s, e, meta_in[slot, e])
        return carry

    lax.fori_loop(0, 4, table_step, 0)

    rl_target = jnp.where(col == 0, left, rel(COLS * dz_rl))
    rl_slot = jnp.where(col == 0, RL, ZRL)

    def fwd_rl(e, j):
        return hop(buf.at[RL, e, j], fwd_send.at[RL, e, j], rl_slot, e, j, core_of(rl_target, core))

    def fwd_lr(e, j):
        return hop(buf.at[LR, e, j], fwd_send.at[LR, e, j], ZLR, e, j, core_of(rel(COLS * dz_lr), core))

    def fwd_lr_on(e, j):
        return hop(buf.at[LR, e, j], fwd2_send.at[e, j], LR, e, j, core_of(right, core))

    def arrived(s, e, j):
        hop(buf.at[s, e, j], fwd_send.at[RL, e, j], s, e, j, {"snp": sibling}).wait_recv()

    def step(t, carry):
        @pl.when(t < parts)
        def _():
            for e in range(2):
                arrived(RL, e, t)
                fwd_rl(e, t).start()

                @pl.when(uses_lr)
                def _(e=e):
                    arrived(LR, e, t)

                    @pl.when(col == 1)
                    def _():
                        fwd_lr_on(e, t).start()
                    fwd_lr(e, t).start()

        def stream(s, inner):
            j = jnp.where(s >= ZRL, t - 1, t)

            @pl.when(uses(s) & (j >= 0) & (j < parts))
            def _():
                @pl.when(s >= ZRL)
                def _():
                    for e in range(2):
                        arrived(s, e, j)
                batch(s, j, j == 0)

                @pl.when(j == parts - 1)
                def _():
                    for e in range(2):
                        part_copy(s, e).start()
            return inner

        lax.fori_loop(0, 4, stream, 0)
        return carry

    lax.fori_loop(0, parts + 1, step, 0)

    def put(tile, at):
        @pl.when((at >= 0) & (at <= 2 * REACH))
        def _():
            out[:, pl.ds(pl.multiple_of(at * LANES, LANES), LANES)] = tile

    def finished(s, e):
        part_arrived(s, e)
        tile = (acc[s, e, 0] + part[s, e]) / samples
        near = jnp.abs(place_of[s, e] - pos[...]) <= BAND_BP
        return jnp.where(near, tile, jnp.zeros_like(tile))

    def mirror_copy(s, e, offset):
        k = core if e == 0 else 1 - core
        return pltpu.make_async_remote_copy(
            src_ref=mir_out.at[s, e], dst_ref=mir_in.at[3 - offset, e], send_sem=mir_send.at[s, e],
            recv_sem=mir_recv.at[3 - offset, e], device_id=core_of(rel(offset), k), device_id_type=MESH)

    def column_of(offset, e):
        k = core if e == 0 else 1 - core
        return 2 * (offset + 3) + k - core

    def finish_step(s, carry):
        @pl.when(uses(s))
        def _():
            offset = offset_of(s)
            for e in range(2):
                tile = finished(s, e)
                mir_out[s, e] = tile.astype(jnp.bfloat16)
                mirror_copy(s, e, offset).start()
                put(tile.T, column_of(offset, e))
        return carry

    lax.fori_loop(0, 4, finish_step, 0)
    for e in range(2):
        put(finished(OWN, e).T, column_of(0, e))

    for offset, cols in OWNERS:
        @pl.when(any_of(col, cols))
        def _(offset=offset):
            for e in range(2):
                pltpu.make_async_remote_copy(
                    src_ref=mir_out.at[0, e], dst_ref=mir_in.at[3 + offset, e], send_sem=mir_send.at[0, e],
                    recv_sem=mir_recv.at[3 + offset, e], device_id={"snp": sibling},
                    device_id_type=MESH).wait_recv()
                put(mir_in[3 + offset, e].astype(jnp.float32), column_of(offset, e))

    for way, sends in ((RL, sends_left), (LR, sends_right)):
        @pl.when(sends)
        def _(way=way):
            for j in range(parts):
                for e in range(2):
                    x_hop(e, j, way).wait_send()
    for j in range(parts):
        to_sibling(j).wait_send()
        for e in range(2):
            fwd_rl(e, j).wait_send()

    @pl.when(uses_lr)
    def _():
        for j in range(parts):
            for e in range(2):
                fwd_lr(e, j).wait_send()

    @pl.when(col == 1)
    def _():
        for j in range(parts):
            for e in range(2):
                fwd_lr_on(e, j).wait_send()
    meta_copy(0, 1).wait_send()
    for offset, cols in OWNERS:
        @pl.when(any_of(col, cols))
        def _(offset=offset):
            for e in range(2):
                meta_copy(offset, e).wait_send()
    for e in range(2):
        part_copy(OWN, e).wait_send()

    def drain(s, carry):
        @pl.when(uses(s))
        def _():
            for e in range(2):
                part_copy(s, e).wait_send()
                mirror_copy(s, e, offset_of(s)).wait_send()
        return carry

    lax.fori_loop(0, 4, drain, 0)


def per_device(genotypes, positions):
    devices = lax.axis_size("snp")
    rows, words = genotypes.shape
    parts = words // (2 * LANES)
    piece = (rows, LANES)
    dma = pltpu.SemaphoreType.DMA
    return pl.pallas_call(
        functools.partial(kernel, devices),
        out_shape=jax.ShapeDtypeStruct((rows, (2 * REACH + 1) * LANES), jnp.float32),
        in_specs=[pl.BlockSpec(memory_space=pltpu.HBM), pl.BlockSpec(memory_space=pltpu.VMEM)],
        out_specs=pl.BlockSpec(memory_space=pltpu.VMEM),
        scratch_shapes=[
            pltpu.VMEM((5, 2, parts) + piece, jnp.int32),
            pltpu.VMEM((parts,) + piece, jnp.int32),
            pltpu.VMEM((parts, CODES * LANES, 2 * rows), jnp.bfloat16),
            pltpu.VMEM((2 * rows, CODES * LANES), jnp.bfloat16),
            pltpu.VMEM((5, 2, 2) + piece, jnp.float32),
            pltpu.VMEM((5, 2) + piece, jnp.float32),
            pltpu.VMEM((5, 2, 3) + piece, jnp.bfloat16),
            pltpu.VMEM((5, 2) + piece, jnp.int32),
            pltpu.VMEM((2, 3) + piece, jnp.bfloat16),
            pltpu.VMEM((8, LANES), jnp.int32),
            pltpu.VMEM((7, 2, 8, LANES), jnp.int32),
            pltpu.VMEM((4, 2) + piece, jnp.bfloat16),
            pltpu.VMEM((7, 2) + piece, jnp.bfloat16),
            dma((2, parts)),
            dma((2, 2, parts)),
            dma((2, 2, parts)),
            dma((2, parts)),
            dma((5, 2, parts)),
            dma((7, 2)),
            dma((7, 2)),
            dma((parts,)),
            dma((5, 2)),
            dma((5, 2)),
            dma((4, 2)),
            dma((7, 2)),
        ],
        compiler_params=pltpu.CompilerParams(
            collective_id=0, has_side_effects=True, vmem_limit_bytes=40 * 1024 * 1024
        ),
    )(genotypes, positions.reshape(1, rows))


def solution(mesh):
    return jax.shard_map(
        per_device,
        mesh=mesh,
        in_specs=(P(("arm", "snp"), None), P(("arm", "snp"))),
        out_specs=P(("arm", "snp"), None),
        check_vma=False,
    )
```

```python
import functools

import jax
import jax.numpy as jnp
from jax import lax
from jax.experimental import pallas as pl
from jax.experimental.pallas import tpu as pltpu
from jax.sharding import PartitionSpec as P

REACH = 6
BAND_BP = 1000000
COLS = 4
LANES = 128
CODES = 16
RL, LR, ZRL, ZLR, OWN = range(5)
MESH = pl.DeviceIdType.MESH
I16 = jnp.int16
GROUP = 16
OWNERS = ((1, (0, 3)), (-1, (2, 3)), (2, (0, 1)), (-2, (0, 1)), (3, (2, 3)), (-3, (0, 3)))


def any_of(col, cols):
    hit = col == cols[0]
    for c in cols[1:]:
        hit = hit | (col == c)
    return hit


def lookup(half, bit, v0, v1, v2, zero):
    high = 2 << bit
    low_set = (half & I16(1 << bit)) != I16(0)
    high_set = (half & I16(high if high < 32768 else -32768)) != I16(0)
    return jnp.where(high_set, jnp.where(low_set, zero, v2), jnp.where(low_set, v1, v0))


def values_of(missing, dosage, samples):
    tally = samples - missing.astype(jnp.float32)
    allele = (dosage.astype(jnp.float32) + 1.0) / (2.0 * tally + 2.0)
    spread = lax.rsqrt(2.0 * allele * (1.0 - allele))
    return [(code - 2.0 * allele) * spread for code in (0.0, 1.0, 2.0)]


def kernel(devices, geno, pos_hbm, out, pos, buf, xbuf, own_t, panel, acc, part, tab, place_of,
           lane_tab, meta_out, meta_in, mir_out, mir_in,
           lane_val, late_sem, load_sem, pos_sem, x_send, fwd_send, fwd2_send, arrive, meta_send, meta_recv, sib_send,
           part_send, part_recv, mir_send, mir_recv):
    rows = pos_hbm.shape[1]
    words = geno.shape[1]
    parts = words // (2 * LANES)
    samples = float(words * CODES)
    me = lax.axis_index("snp")
    chips = devices // 2
    core = lax.rem(me, 2)
    chip = me // 2
    col = lax.rem(chip, COLS)
    base = chip - col

    def exists(offset):
        return (chip + offset >= 0) & (chip + offset < chips)

    left = base + lax.rem(col + COLS - 1, COLS)
    right = base + lax.rem(col + 1, COLS)
    sibling = me + 1 - 2 * core

    def core_of(c, k):
        return {"snp": c * 2 + k}

    barrier = pltpu.get_barrier_semaphore()

    first = me == 0

    def greet(c):
        @pl.when(~first)
        def _():
            for k in range(2):
                pl.semaphore_signal(barrier, inc=1, device_id=core_of(c, k), device_id_type=MESH)

    def greets(c):
        return 2 - ((c == 0) & ~first).astype(jnp.int32)

    @pl.when(~first)
    def _():
        pl.semaphore_signal(barrier, inc=1, device_id={"snp": sibling}, device_id_type=MESH)
    greet(left)
    greet(right)
    greeted = greets(left) + greets(right) + (me != 1).astype(jnp.int32)
    for offset in (COLS, -COLS, 1, -1, 2, -2, 3, -3):
        @pl.when(exists(offset))
        def _(offset=offset):
            greet(chip + offset)
        greeted = greeted + greets(chip + offset) * exists(offset).astype(jnp.int32)

    loads = []
    for e in range(2):
        half = core if e == 0 else 1 - core
        for j in range(parts):
            lane = pl.multiple_of((half * parts + j) * LANES, LANES)
            dst = buf.at[OWN, 0, j] if e == 0 else xbuf.at[j]
            loads.append(pltpu.make_async_copy(geno.at[:, pl.ds(lane, LANES)], dst, load_sem.at[e, j]))
            loads[-1].start()

    pos_load = pltpu.make_async_copy(pos_hbm, pos, pos_sem)
    pos_load.start()

    def own_piece(e, j):
        return buf.at[OWN, 0, j] if e == 0 else xbuf.at[j]


    sends_left = col >= 1
    sends_right = (col == 0) | (col == 3)
    uses_lr = col <= 2
    top = chip < COLS
    lag = jnp.where(top, parts + 1, 0)
    late_end = top & (col == 3)
    dz_rl = jnp.where(col == 3, -1, 1)
    dz_lr = jnp.where(col == 0, 1, -1)
    off_rl = jnp.where(col == 3, -2, 1)
    off_lr = jnp.where(col == 0, 3, jnp.where(col == 1, -1, -2))
    off_zrl = off_rl - COLS * dz_rl
    off_zlr = off_lr - COLS * dz_lr

    def offset_of(s):
        return jnp.where(s == RL, off_rl, jnp.where(s == LR, off_lr, jnp.where(s == ZRL, off_zrl, off_zlr)))

    z_rl = exists(-COLS * dz_rl)
    z_lr = exists(-COLS * dz_lr)

    def uses(s):
        along = jnp.where((s == RL) | (s == ZRL), col >= 1, col <= 2)
        return along & ((s < ZRL) | jnp.where(s == ZRL, z_rl, z_lr))

    for copy in loads:
        copy.wait()
    pos_load.wait()
    missing = jnp.zeros((rows, LANES), jnp.int32)
    dosage = jnp.zeros((rows, LANES), jnp.int32)
    for e in range(2):
        for j in range(parts):
            word = own_piece(e, j)[...]
            low = word & 0x55555555
            high = lax.shift_right_logical(word, 1) & 0x55555555
            gone = lax.population_count(low & high)
            missing = missing + gone
            dosage = dosage + lax.population_count(low) + 2 * lax.population_count(high) - 3 * gone
    counts = []
    for x in (missing, dosage):
        total = jnp.broadcast_to(jnp.sum(x, axis=1, keepdims=True), (rows, LANES))
        counts.append(total.T[0:1])
    meta_out[0:1] = pos[...]
    meta_out[1:2] = counts[0]
    meta_out[2:3] = counts[1]
    meta_out[3:8] = jnp.zeros((5, LANES), jnp.int32)

    def fill_tables(s, e, counts8):
        place_of[s, e] = jnp.broadcast_to(counts8.T[:, 0:1], (rows, LANES))
        for i, v in enumerate(values_of(counts8[1:2], counts8[2:3], samples)):
            lane_val[i:i + 1] = v
        columns = lane_val[...].T
        for i in range(3):
            tab[s, e, i] = jnp.broadcast_to(columns[:, i:i + 1], (rows, LANES)).astype(jnp.bfloat16)

    def lanes_of(e, counts8):
        for i, v in enumerate(values_of(counts8[1:2], counts8[2:3], samples)):
            lane_tab[e, i] = jnp.broadcast_to(v, (GROUP, LANES)).astype(jnp.bfloat16)

    def halves_of(word):
        return word.astype(I16), lax.shift_right_logical(word, 16).astype(I16)

    def turn(e, j):
        turned = buf[OWN, e, j].T
        v0, v1, v2 = (lane_tab[e, i] for i in range(3))
        zero = jnp.zeros_like(v0)
        for g in range(0, LANES, GROUP):
            halves = halves_of(turned[g:g + GROUP])
            for q in range(CODES):
                own_t[j, q * LANES + g:q * LANES + g + GROUP, e * rows:(e + 1) * rows] = lookup(
                    halves[q // 8], 2 * (q % 8), v0, v1, v2, zero)

    lane_val[...] = jnp.zeros_like(lane_val)
    fill_tables(OWN, 0, meta_out[...])
    lanes_of(0, meta_out[...])

    def turn_own(j, carry):
        turn(0, j)
        return carry

    lax.fori_loop(0, parts, turn_own, 0)
    pl.semaphore_wait(barrier, greeted)

    @pl.when(first)
    def _():
        pl.semaphore_signal(late_sem, inc=1, device_id={"snp": sibling}, device_id_type=MESH)
        for c in range(1, COLS):
            for k in range(2):
                pl.semaphore_signal(late_sem, inc=1, device_id=core_of(c, k), device_id_type=MESH)

    def meta_copy(offset, e):
        k = core if e == 0 else 1 - core
        return pltpu.make_async_remote_copy(
            src_ref=meta_out, dst_ref=meta_in.at[3 - offset, e], send_sem=meta_send.at[3 + offset, e],
            recv_sem=meta_recv.at[3 - offset, e],
            device_id={"snp": sibling} if offset == 0 else core_of(chip + offset, k), device_id_type=MESH)

    for offset, cols in OWNERS:
        waits = late_end if offset == -3 else False

        @pl.when(any_of(col, cols) & exists(offset) & ~jnp.bool_(waits))
        def _(offset=offset):
            for e in range(2):
                meta_copy(offset, e).start()

    def hop(src, send_sem, s, e, j, target):
        return pltpu.make_async_remote_copy(
            src_ref=src, dst_ref=buf.at[s, e, j], send_sem=send_sem, recv_sem=arrive.at[s, e, j],
            device_id=target, device_id_type=MESH)

    def x_hop(e, j, way):
        c = jnp.where(col == 1, base + 3, left) if way == RL else right
        return hop(own_piece(e, j), x_send.at[way, e, j], way, e, j, core_of(c, core if e == 0 else 1 - core))

    def x_hop_down(e, j):
        return hop(own_piece(e, j), fwd_send.at[LR, e, j], ZLR, e, j,
                   core_of(chip + 1, core if e == 0 else 1 - core))

    def to_first(e, way):
        return late_end & (core == e) if way == LR else False

    def to_sibling(j):
        return hop(xbuf.at[j], sib_send.at[j], OWN, 1, j, {"snp": sibling})

    def greet_sibling():
        meta_copy(0, 1).start()
        for j in range(parts):
            to_sibling(j).start()

    @pl.when(me != 1)
    def _():
        greet_sibling()

    for way, sends in ((RL, sends_left), (LR, sends_right)):
        for j in range(parts):
            for e in range(2):
                @pl.when(sends & ~jnp.bool_(to_first(e, way)))
                def _(way=way, e=e, j=j):
                    x_hop(e, j, way).start()

    @pl.when(late_end)
    def _():
        for j in range(parts):
            for e in range(2):
                x_hop_down(e, j).start()

    out[...] = jnp.zeros_like(out)

    def batch(s, j):
        for e in range(2):
            for g in range(0, rows, GROUP):
                halves = halves_of(buf[s, e, j, g:g + GROUP])
                v0, v1, v2 = (tab[s, e, i, g:g + GROUP] for i in range(3))
                zero = jnp.zeros_like(v0)
                for q in range(CODES):
                    panel[e * rows + g:e * rows + g + GROUP, q * LANES:(q + 1) * LANES] = lookup(
                        halves[q // 8], 2 * (q % 8), v0, v1, v2, zero)
        product = lax.dot_general(panel[...], own_t[j], (((1,), (0,)), ((), ())),
                                  preferred_element_type=jnp.float32)
        for e in range(2):
            for c in range(2):
                tile = product[e * rows:(e + 1) * rows, c * LANES:(c + 1) * LANES]
                acc[s, e, c] = jnp.where(j == 0, tile, acc[s, e, c] + tile)

    def meta_arrived(slot, e):
        pltpu.make_async_remote_copy(
            src_ref=meta_out, dst_ref=meta_in.at[slot, e], send_sem=meta_send.at[slot, e],
            recv_sem=meta_recv.at[slot, e], device_id={"snp": sibling}, device_id_type=MESH).wait_recv()

    @pl.when(me == 1)
    def _():
        pl.semaphore_wait(late_sem, 1)
        greet_sibling()

    meta_arrived(3, 1)
    fill_tables(OWN, 1, meta_in[3, 1])
    lanes_of(1, meta_in[3, 1])

    def part_copy(s, e):
        return pltpu.make_async_remote_copy(
            src_ref=acc.at[s, e, 1], dst_ref=part.at[s, 1 - e], send_sem=part_send.at[s, e],
            recv_sem=part_recv.at[s, 1 - e], device_id={"snp": sibling}, device_id_type=MESH)

    def part_arrived(s, e):
        pltpu.make_async_remote_copy(
            src_ref=acc.at[s, e, 1], dst_ref=part.at[s, e], send_sem=part_send.at[s, e],
            recv_sem=part_recv.at[s, e], device_id={"snp": sibling}, device_id_type=MESH).wait_recv()

    def own_step(j):
        to_sibling(j).wait_recv()
        turn(1, j)
        batch(OWN, j)

        @pl.when(j == parts - 1)
        def _():
            for e in range(2):
                part_copy(OWN, e).start()

    passes_rl = (col >= 1) & exists(COLS * dz_rl)
    passes_lr = uses_lr & exists(COLS * dz_lr) & (chip > 0)

    def fwd_rl(e, j):
        return hop(buf.at[RL, e, j], fwd_send.at[RL, e, j], ZRL, e, j, core_of(chip + COLS * dz_rl, core))

    def fwd_lr(e, j):
        return hop(buf.at[LR, e, j], fwd_send.at[LR, e, j], ZLR, e, j, core_of(chip + COLS * dz_lr, core))

    def fwd_lr_on(e, j):
        return hop(buf.at[LR, e, j], fwd2_send.at[e, j], LR, e, j, core_of(right, core))

    def arrived(s, e, j):
        hop(buf.at[s, e, j], fwd_send.at[RL, e, j], s, e, j, {"snp": sibling}).wait_recv()

    def put(tile, at):
        @pl.when((at >= 0) & (at <= 2 * REACH))
        def _():
            out[:, pl.ds(pl.multiple_of(at * LANES, LANES), LANES)] = tile

    def finished(s, e):
        part_arrived(s, e)
        tile = (acc[s, e, 0] + part[s, e]) / samples
        near = jnp.abs(place_of[s, e] - pos[...]) <= BAND_BP
        return jnp.where(near, tile, jnp.zeros_like(tile))

    def mirror_copy(s, e, offset):
        k = core if e == 0 else 1 - core
        return pltpu.make_async_remote_copy(
            src_ref=mir_out.at[s, e], dst_ref=mir_in.at[3 - offset, e], send_sem=mir_send.at[s, e],
            recv_sem=mir_recv.at[3 - offset, e], device_id=core_of(chip + offset, k), device_id_type=MESH)

    def column_of(offset, e):
        k = core if e == 0 else 1 - core
        return 2 * (offset + 3) + k - core

    def finish(s):
        offset = offset_of(s)
        for e in range(2):
            tile = finished(s, e)
            mir_out[s, e] = tile.astype(jnp.bfloat16)
            mirror_copy(s, e, offset).start()
            put(tile.T, column_of(offset, e))

    def finish_some(low, high, wanted):
        def one(s, carry):
            @pl.when(wanted(s) & uses(s))
            def _():
                finish(s)
            return carry

        lax.fori_loop(low, high, one, 0)

    def step(t, carry):
        @pl.when((t == parts + 1) & (col >= 1))
        def _():
            pl.semaphore_wait(late_sem, 1)

            @pl.when(late_end)
            def _():
                for e in range(2):
                    meta_copy(-3, e).start()
                for j in range(parts):
                    for e in range(2):
                        @pl.when(to_first(e, LR))
                        def _(e=e, j=j):
                            x_hop(e, j, LR).start()

        behind = t - lag
        for e in range(2):
            @pl.when((t >= 0) & (t < parts) & (col >= 1))
            def _(e=e):
                arrived(RL, e, t)

                @pl.when(passes_rl)
                def _():
                    fwd_rl(e, t).start()

            @pl.when((behind >= 0) & (behind < parts) & uses_lr)
            def _(e=e):
                arrived(LR, e, behind)

                @pl.when(col == 1)
                def _():
                    fwd_lr_on(e, behind).start()

                @pl.when(passes_lr)
                def _():
                    fwd_lr(e, behind).start()

        @pl.when(t < parts - 1)
        def _():
            own_step(t + 1)

        @pl.when(t == parts)
        def _():
            finish_some(RL, ZRL, lambda s: (s == RL) | (lag == 0))
            for e in range(2):
                put(finished(OWN, e).T, column_of(0, e))

        @pl.when(t == parts + 1)
        def _():
            finish_some(ZRL, OWN, lambda s: s >= ZRL)

        def stream(s, inner):
            j = jnp.where(s >= ZRL, t - 1, jnp.where(s == LR, behind, t))

            @pl.when(uses(s) & (j >= 0) & (j < parts))
            def _():
                @pl.when(j == 0)
                def _():
                    slot = offset_of(s) + 3
                    for e in range(2):
                        meta_arrived(slot, e)
                        fill_tables(s, e, meta_in[slot, e])

                @pl.when(s >= ZRL)
                def _():
                    for e in range(2):
                        arrived(s, e, j)
                batch(s, j)

                @pl.when(j == parts - 1)
                def _():
                    for e in range(2):
                        part_copy(s, e).start()
            return inner

        lax.fori_loop(RL, OWN, stream, 0)
        return carry

    lax.fori_loop(-1, parts + 1 + lag, step, 0)
    finish_some(RL, OWN, lambda s: jnp.where(lag == 0, s >= ZRL, s == LR))

    for offset, cols in OWNERS:
        @pl.when(any_of(col, cols) & exists(offset))
        def _(offset=offset):
            for e in range(2):
                pltpu.make_async_remote_copy(
                    src_ref=mir_out.at[0, e], dst_ref=mir_in.at[3 + offset, e], send_sem=mir_send.at[0, e],
                    recv_sem=mir_recv.at[3 + offset, e], device_id={"snp": sibling},
                    device_id_type=MESH).wait_recv()
                put(mir_in[3 + offset, e].astype(jnp.float32), column_of(offset, e))

    for way, sends in ((RL, sends_left), (LR, sends_right)):
        @pl.when(sends)
        def _(way=way):
            for j in range(parts):
                for e in range(2):
                    x_hop(e, j, way).wait_send()
    for j in range(parts):
        to_sibling(j).wait_send()

    @pl.when(passes_rl)
    def _():
        for j in range(parts):
            for e in range(2):
                fwd_rl(e, j).wait_send()

    @pl.when(passes_lr | late_end)
    def _():
        for j in range(parts):
            for e in range(2):
                fwd_lr(e, j).wait_send()

    @pl.when(col == 1)
    def _():
        for j in range(parts):
            for e in range(2):
                fwd_lr_on(e, j).wait_send()
    meta_copy(0, 1).wait_send()
    for offset, cols in OWNERS:
        @pl.when(any_of(col, cols) & exists(offset))
        def _(offset=offset):
            for e in range(2):
                meta_copy(offset, e).wait_send()
    for e in range(2):
        part_copy(OWN, e).wait_send()

    def drain(s, carry):
        @pl.when(uses(s))
        def _():
            for e in range(2):
                part_copy(s, e).wait_send()
                mirror_copy(s, e, offset_of(s)).wait_send()
        return carry

    lax.fori_loop(0, 4, drain, 0)


def per_device(genotypes, positions):
    devices = lax.axis_size("snp")
    rows, words = genotypes.shape
    parts = words // (2 * LANES)
    piece = (rows, LANES)
    dma = pltpu.SemaphoreType.DMA
    return pl.pallas_call(
        functools.partial(kernel, devices),
        out_shape=pltpu.VMEM((rows, (2 * REACH + 1) * LANES), jnp.float32),
        in_specs=[pl.BlockSpec(memory_space=pltpu.HBM)] * 2,
        out_specs=pl.BlockSpec(memory_space=pltpu.VMEM),
        scratch_shapes=[
            pltpu.VMEM((1, rows), jnp.int32),
            pltpu.VMEM((5, 2, parts) + piece, jnp.int32),
            pltpu.VMEM((parts,) + piece, jnp.int32),
            pltpu.VMEM((parts, CODES * LANES, 2 * rows), jnp.bfloat16),
            pltpu.VMEM((2 * rows, CODES * LANES), jnp.bfloat16),
            pltpu.VMEM((5, 2, 2) + piece, jnp.float32),
            pltpu.VMEM((5, 2) + piece, jnp.float32),
            pltpu.VMEM((5, 2, 3) + piece, jnp.bfloat16),
            pltpu.VMEM((5, 2) + piece, jnp.int32),
            pltpu.VMEM((2, 3, GROUP, LANES), jnp.bfloat16),
            pltpu.VMEM((8, LANES), jnp.int32),
            pltpu.VMEM((7, 2, 8, LANES), jnp.int32),
            pltpu.VMEM((4, 2) + piece, jnp.bfloat16),
            pltpu.VMEM((7, 2) + piece, jnp.bfloat16),
            pltpu.VMEM((8, LANES), jnp.float32),
            pltpu.SemaphoreType.REGULAR,
            dma((2, parts)),
            dma,
            dma((2, 2, parts)),
            dma((2, 2, parts)),
            dma((2, parts)),
            dma((5, 2, parts)),
            dma((7, 2)),
            dma((7, 2)),
            dma((parts,)),
            dma((5, 2)),
            dma((5, 2)),
            dma((4, 2)),
            dma((7, 2)),
        ],
        compiler_params=pltpu.CompilerParams(
            collective_id=0, has_side_effects=True, vmem_limit_bytes=60 * 1024 * 1024
        ),
    )(genotypes, positions.reshape(1, rows))


def solution(mesh):
    return jax.shard_map(
        per_device,
        mesh=mesh,
        in_specs=(P(("arm", "snp"), None), P(("arm", "snp"))),
        out_specs=P(("arm", "snp"), None),
        check_vma=False,
    )
```

```python
import functools

import jax
import jax.numpy as jnp
from jax import lax
from jax.experimental import pallas as pl
from jax.experimental.pallas import tpu as pltpu
from jax.sharding import PartitionSpec as P

REACH = 6
BAND_BP = 1000000
COLS = 4
LANES = 128
CODES = 16
RL, LR, ZRL, ZLR, OWN = range(5)
MESH = pl.DeviceIdType.MESH
I16 = jnp.int16
GROUP = 16
OWNERS = ((1, (0, 3)), (2, (0, 1)), (3, (2, 3)), (-2, (0, 1)), (-1, (2, 3)), (-3, (0, 3)))


def any_of(col, cols):
    hit = col == cols[0]
    for c in cols[1:]:
        hit = hit | (col == c)
    return hit


def lookup(half, bit, v0, v1, v2, zero):
    high = 2 << bit
    low_set = (half & I16(1 << bit)) != I16(0)
    high_set = (half & I16(high if high < 32768 else -32768)) != I16(0)
    return jnp.where(high_set, jnp.where(low_set, zero, v2), jnp.where(low_set, v1, v0))


def values_of(missing, dosage, samples):
    tally = samples - missing.astype(jnp.float32)
    allele = (dosage.astype(jnp.float32) + 1.0) / (2.0 * tally + 2.0)
    spread = lax.rsqrt(2.0 * allele * (1.0 - allele))
    return [(code - 2.0 * allele) * spread for code in (0.0, 1.0, 2.0)]


def kernel(devices, geno, pos_hbm, out, pos, buf, xbuf, own_t, panel, acc, part, tab, place_of,
           lane_tab, meta_out, meta_in, mir_out, mir_in,
           lane_val, late_sem, load_sem, pos_sem, x_send, fwd_send, fwd2_send, arrive, meta_send, meta_recv, sib_send,
           part_send, part_recv, mir_send, mir_recv):
    rows = pos_hbm.shape[1]
    words = geno.shape[1]
    parts = words // (2 * LANES)
    samples = float(words * CODES)
    me = lax.axis_index("snp")
    chips = devices // 2
    core = lax.rem(me, 2)
    chip = me // 2
    col = lax.rem(chip, COLS)
    base = chip - col

    def exists(offset):
        return (chip + offset >= 0) & (chip + offset < chips)

    def owned_at(offset, cols):
        there = any_of(col, cols)
        if offset == 1:
            return there & (chip > 0)
        return there | (chip == 1) if offset == -1 else there

    left = base + lax.rem(col + COLS - 1, COLS)
    right = base + lax.rem(col + 1, COLS)
    sibling = me + 1 - 2 * core

    def core_of(c, k):
        return {"snp": c * 2 + k}

    barrier = pltpu.get_barrier_semaphore()

    first = me == 0

    def greet(c):
        @pl.when(~first)
        def _():
            for k in range(2):
                pl.semaphore_signal(barrier, inc=1, device_id=core_of(c, k), device_id_type=MESH)

    def greets(c):
        return 2 - ((c == 0) & ~first).astype(jnp.int32)

    @pl.when(~first)
    def _():
        pl.semaphore_signal(barrier, inc=1, device_id={"snp": sibling}, device_id_type=MESH)
    greet(left)
    greet(right)
    greeted = greets(left) + greets(right) + (me != 1).astype(jnp.int32)
    for offset in (COLS, -COLS, 1, -1, 2, -2, 3, -3):
        @pl.when(exists(offset))
        def _(offset=offset):
            greet(chip + offset)
        greeted = greeted + greets(chip + offset) * exists(offset).astype(jnp.int32)

    loads = []
    for e in range(2):
        half = core if e == 0 else 1 - core
        for j in range(parts):
            lane = pl.multiple_of((half * parts + j) * LANES, LANES)
            dst = buf.at[OWN, 0, j] if e == 0 else xbuf.at[j]
            loads.append(pltpu.make_async_copy(geno.at[:, pl.ds(lane, LANES)], dst, load_sem.at[e, j]))
            loads[-1].start()

    pos_load = pltpu.make_async_copy(pos_hbm, pos, pos_sem)
    pos_load.start()

    def own_piece(e, j):
        return buf.at[OWN, 0, j] if e == 0 else xbuf.at[j]


    sends_left = col >= 1
    sends_right = (col == 0) | (col == 3)
    uses_rl = (col >= 1) | (chip == 0)
    uses_lr = (col <= 2) & (chip != 1)
    top = chip < COLS

    def lag_of(s):
        late = jnp.where(top, parts + 1, jnp.where(col == 2, 1, 0))
        return jnp.where(s == RL, jnp.where(chip == 0, parts + 1, 0), jnp.where(s == LR, late, jnp.where((s == ZLR) & (col == 2), 2, 1)))

    lag = lag_of(LR)
    steps = parts + 1 + jnp.where(top, parts + 1, jnp.where(col == 2, 2, 1))
    late_end = (chip == 1) | (chip == 3)
    dz_rl = jnp.where(col == 3, -1, 1)
    dz_lr = jnp.where(col == 0, 1, -1)
    off_rl = jnp.where(col == 3, -2, 1)
    off_lr = jnp.where(col == 0, 3, jnp.where(col == 1, -1, -2))
    off_zrl = off_rl - COLS * dz_rl
    off_zlr = off_lr - COLS * dz_lr

    def offset_of(s):
        return jnp.where(s == RL, off_rl, jnp.where(s == LR, off_lr, jnp.where(s == ZRL, off_zrl, off_zlr)))

    z_rl = exists(-COLS * dz_rl)
    z_lr = exists(-COLS * dz_lr)

    def uses(s):
        z = jnp.where(s == ZRL, z_rl & (col >= 1), z_lr & (col <= 2))
        return jnp.where(s == RL, uses_rl, jnp.where(s == LR, uses_lr, z))

    for copy in loads:
        copy.wait()
    pos_load.wait()
    missing = jnp.zeros((rows, LANES), jnp.int32)
    dosage = jnp.zeros((rows, LANES), jnp.int32)
    for e in range(2):
        for j in range(parts):
            word = own_piece(e, j)[...]
            low = word & 0x55555555
            high = lax.shift_right_logical(word, 1) & 0x55555555
            gone = lax.population_count(low & high)
            missing = missing + gone
            dosage = dosage + lax.population_count(low) + 2 * lax.population_count(high) - 3 * gone
    counts = []
    for x in (missing, dosage):
        total = jnp.broadcast_to(jnp.sum(x, axis=1, keepdims=True), (rows, LANES))
        counts.append(total.T[0:1])
    meta_out[0:1] = pos[...]
    meta_out[1:2] = counts[0]
    meta_out[2:3] = counts[1]
    meta_out[3:8] = jnp.zeros((5, LANES), jnp.int32)

    def meta_copy(offset, e):
        k = core if e == 0 else 1 - core
        return pltpu.make_async_remote_copy(
            src_ref=meta_out, dst_ref=meta_in.at[3 - offset, e], send_sem=meta_send.at[3 + offset, e],
            recv_sem=meta_recv.at[3 - offset, e],
            device_id={"snp": sibling} if offset == 0 else core_of(chip + offset, k), device_id_type=MESH)

    def hop(src, send_sem, s, e, j, target):
        return pltpu.make_async_remote_copy(
            src_ref=src, dst_ref=buf.at[s, e, j], send_sem=send_sem, recv_sem=arrive.at[s, e, j],
            device_id=target, device_id_type=MESH)

    def x_hop(e, j, way):
        c = jnp.where(col == 1, base + 3, left) if way == RL else jnp.where(chip == 0, 2, right)
        return hop(own_piece(e, j), x_send.at[way, e, j], way, e, j, core_of(c, core if e == 0 else 1 - core))

    def x_hop_down(e, j):
        return hop(own_piece(e, j), fwd_send.at[LR, e, j], ZLR, e, j,
                   core_of(chip + 1, core if e == 0 else 1 - core))

    def to_first(e, way):
        return (chip == 3) & (core == e) if way == LR else False

    def x_hop_first(e, j):
        return hop(own_piece(e, j), x_send.at[LR, e, j], RL, e, j, core_of(0, core if e == 0 else 1 - core))

    def to_sibling(j):
        return hop(xbuf.at[j], sib_send.at[j], OWN, 1, j, {"snp": sibling})

    def greet_sibling():
        meta_copy(0, 1).start()
        for j in range(parts):
            to_sibling(j).start()

    def send_first():
        for offset, cols in OWNERS:
            waits = chip + offset == 0 if offset in (-1, -3) else False

            @pl.when(owned_at(offset, cols) & exists(offset) & ~jnp.bool_(waits))
            def _(offset=offset):
                for e in range(2):
                    meta_copy(offset, e).start()

        @pl.when(me != 1)
        def _():
            greet_sibling()

        for way, sends in ((RL, sends_left), (LR, sends_right)):
            for j in range(parts):
                for e in range(2):
                    @pl.when(sends & ~jnp.bool_(to_first(e, way)))
                    def _(way=way, e=e, j=j):
                        x_hop(e, j, way).start()

        @pl.when(chip == 3)
        def _():
            for j in range(parts):
                for e in range(2):
                    x_hop_down(e, j).start()

        for e in range(2):
            @pl.when((chip == 1) & (core != e))
            def _(e=e):
                for j in range(parts):
                    x_hop_first(e, j).start()

    @pl.when(first)
    def _():
        pl.semaphore_wait(barrier, greeted)
        pl.semaphore_signal(late_sem, inc=1, device_id={"snp": sibling}, device_id_type=MESH)
        for c in range(1, COLS):
            for k in range(2):
                pl.semaphore_signal(late_sem, inc=1, device_id=core_of(c, k), device_id_type=MESH)
        send_first()

    def fill_tables(s, e, counts8):
        place_of[s, e] = jnp.broadcast_to(counts8.T[:, 0:1], (rows, LANES))
        for i, v in enumerate(values_of(counts8[1:2], counts8[2:3], samples)):
            lane_val[i:i + 1] = v
        columns = lane_val[...].T
        for i in range(3):
            tab[s, e, i] = jnp.broadcast_to(columns[:, i:i + 1], (rows, LANES)).astype(jnp.bfloat16)

    def lanes_of(e, counts8):
        for i, v in enumerate(values_of(counts8[1:2], counts8[2:3], samples)):
            lane_tab[e, i] = jnp.broadcast_to(v, (GROUP, LANES)).astype(jnp.bfloat16)

    def halves_of(word):
        return word.astype(I16), lax.shift_right_logical(word, 16).astype(I16)

    def turn(e, j):
        turned = buf[OWN, e, j].T
        v0, v1, v2 = (lane_tab[e, i] for i in range(3))
        zero = jnp.zeros_like(v0)
        for g in range(0, LANES, GROUP):
            halves = halves_of(turned[g:g + GROUP])
            for q in range(CODES):
                own_t[j, q * LANES + g:q * LANES + g + GROUP, e * rows:(e + 1) * rows] = lookup(
                    halves[q // 8], 2 * (q % 8), v0, v1, v2, zero)

    lane_val[...] = jnp.zeros_like(lane_val)
    acc[...] = jnp.zeros_like(acc)
    fill_tables(OWN, 0, meta_out[...])
    lanes_of(0, meta_out[...])

    def turn_own(j, carry):
        turn(0, j)
        return carry

    lax.fori_loop(0, parts, turn_own, 0)
    @pl.when(~first)
    def _():
        pl.semaphore_wait(barrier, greeted)
        send_first()

    out[...] = jnp.zeros_like(out)

    def batch(s, j):
        for e in range(2):
            for g in range(0, rows, GROUP):
                halves = halves_of(buf[s, e, j, g:g + GROUP])
                v0, v1, v2 = (tab[s, e, i, g:g + GROUP] for i in range(3))
                zero = jnp.zeros_like(v0)
                for q in range(CODES):
                    panel[e * rows + g:e * rows + g + GROUP, q * LANES:(q + 1) * LANES] = lookup(
                        halves[q // 8], 2 * (q % 8), v0, v1, v2, zero)
        product = lax.dot_general(panel[...], own_t[j], (((1,), (0,)), ((), ())),
                                  preferred_element_type=jnp.float32)
        for e in range(2):
            for c in range(2):
                tile = product[e * rows:(e + 1) * rows, c * LANES:(c + 1) * LANES]
                acc[s, e, c] += tile

    def meta_arrived(slot, e):
        pltpu.make_async_remote_copy(
            src_ref=meta_out, dst_ref=meta_in.at[slot, e], send_sem=meta_send.at[slot, e],
            recv_sem=meta_recv.at[slot, e], device_id={"snp": sibling}, device_id_type=MESH).wait_recv()

    @pl.when(me == 1)
    def _():
        pl.semaphore_wait(late_sem, 1)
        greet_sibling()

    meta_arrived(3, 1)
    fill_tables(OWN, 1, meta_in[3, 1])
    lanes_of(1, meta_in[3, 1])

    def part_copy(s, e):
        return pltpu.make_async_remote_copy(
            src_ref=acc.at[s, e, 1], dst_ref=part.at[s, 1 - e], send_sem=part_send.at[s, e],
            recv_sem=part_recv.at[s, 1 - e], device_id={"snp": sibling}, device_id_type=MESH)

    def part_arrived(s, e):
        pltpu.make_async_remote_copy(
            src_ref=acc.at[s, e, 1], dst_ref=part.at[s, e], send_sem=part_send.at[s, e],
            recv_sem=part_recv.at[s, e], device_id={"snp": sibling}, device_id_type=MESH).wait_recv()

    def own_step(j):
        to_sibling(j).wait_recv()
        turn(1, j)
        batch(OWN, j)

        @pl.when(j == parts - 1)
        def _():
            for e in range(2):
                part_copy(OWN, e).start()

    passes_rl = (col >= 1) & exists(COLS * dz_rl)
    passes_lr = uses_lr & exists(COLS * dz_lr) & (chip > 0)
    passes_on = (col == 1) & (chip != 1)

    def fwd_rl(e, j):
        return hop(buf.at[RL, e, j], fwd_send.at[RL, e, j], ZRL, e, j, core_of(chip + COLS * dz_rl, core))

    def fwd_lr(e, j):
        return hop(buf.at[LR, e, j], fwd_send.at[LR, e, j], ZLR, e, j, core_of(chip + COLS * dz_lr, core))

    def fwd_lr_on(e, j):
        return hop(buf.at[LR, e, j], fwd2_send.at[e, j], LR, e, j, core_of(right, core))

    def arrived(s, e, j):
        hop(buf.at[s, e, j], fwd_send.at[RL, e, j], s, e, j, {"snp": sibling}).wait_recv()

    def put(tile, at):
        @pl.when((at >= 0) & (at <= 2 * REACH))
        def _():
            out[:, pl.ds(pl.multiple_of(at * LANES, LANES), LANES)] = tile

    def finished(s, e):
        part_arrived(s, e)
        tile = (acc[s, e, 0] + part[s, e]) / samples
        near = jnp.abs(place_of[s, e] - pos[...]) <= BAND_BP
        return jnp.where(near, tile, jnp.zeros_like(tile))

    def mirror_copy(s, e, offset):
        k = core if e == 0 else 1 - core
        return pltpu.make_async_remote_copy(
            src_ref=mir_out.at[s, e], dst_ref=mir_in.at[3 - offset, e], send_sem=mir_send.at[s, e],
            recv_sem=mir_recv.at[3 - offset, e], device_id=core_of(chip + offset, k), device_id_type=MESH)

    def column_of(offset, e):
        k = core if e == 0 else 1 - core
        return 2 * (offset + 3) + k - core

    def finish(s):
        offset = offset_of(s)
        for e in range(2):
            tile = finished(s, e)
            mir_out[s, e] = tile.astype(jnp.bfloat16)
            mirror_copy(s, e, offset).start()
            put(tile.T, column_of(offset, e))

    def step(t, carry):
        @pl.when(top & (col >= 1) & (t == parts))
        def _():
            pl.semaphore_wait(late_sem, 1)

            for offset in (-1, -3):
                @pl.when(late_end & (chip + offset == 0))
                def _(offset=offset):
                    for e in range(2):
                        meta_copy(offset, e).start()
            for e in range(2):
                @pl.when((chip == 1) & (core == e))
                def _(e=e):
                    for j in range(parts):
                        x_hop_first(e, j).start()

                @pl.when((chip == 3) & (core == e))
                def _(e=e):
                    for j in range(parts):
                        x_hop(e, j, LR).start()

        behind = t - lag
        for e in range(2):
            at_rl = t - lag_of(RL)

            @pl.when((at_rl >= 0) & (at_rl < parts) & uses_rl)
            def _(e=e, at_rl=at_rl):
                arrived(RL, e, at_rl)

                @pl.when(passes_rl)
                def _():
                    fwd_rl(e, at_rl).start()

            @pl.when((behind >= 0) & (behind < parts) & uses_lr)
            def _(e=e):
                arrived(LR, e, behind)

                @pl.when(passes_on)
                def _():
                    fwd_lr_on(e, behind).start()

                @pl.when(passes_lr)
                def _():
                    fwd_lr(e, behind).start()

        @pl.when(t < parts - 1)
        def _():
            own_step(t + 1)

        @pl.when(t == parts)
        def _():
            for e in range(2):
                put(finished(OWN, e).T, column_of(0, e))

        def stream(s, inner):
            j = t - lag_of(s)

            @pl.when(uses(s) & (j >= 0) & (j < parts))
            def _():
                @pl.when(j == 0)
                def _():
                    slot = offset_of(s) + 3
                    for e in range(2):
                        meta_arrived(slot, e)
                        fill_tables(s, e, meta_in[slot, e])

                @pl.when(s >= ZRL)
                def _():
                    for e in range(2):
                        arrived(s, e, j)
                batch(s, j)

                @pl.when(j == parts - 1)
                def _():
                    for e in range(2):
                        part_copy(s, e).start()

            @pl.when(uses(s) & (j == parts))
            def _():
                finish(s)
            return inner

        lax.fori_loop(RL, OWN, stream, 0)
        return carry

    lax.fori_loop(-1, steps, step, 0)

    for offset, cols in OWNERS:
        @pl.when(owned_at(offset, cols) & exists(offset))
        def _(offset=offset):
            for e in range(2):
                pltpu.make_async_remote_copy(
                    src_ref=mir_out.at[0, e], dst_ref=mir_in.at[3 + offset, e], send_sem=mir_send.at[0, e],
                    recv_sem=mir_recv.at[3 + offset, e], device_id={"snp": sibling},
                    device_id_type=MESH).wait_recv()
                put(mir_in[3 + offset, e].astype(jnp.float32), column_of(offset, e))

    for way, sends in ((RL, sends_left), (LR, sends_right | (chip == 1))):
        @pl.when(sends)
        def _(way=way):
            for j in range(parts):
                for e in range(2):
                    x_hop(e, j, way).wait_send()
    for j in range(parts):
        to_sibling(j).wait_send()

    @pl.when(passes_rl)
    def _():
        for j in range(parts):
            for e in range(2):
                fwd_rl(e, j).wait_send()

    @pl.when(passes_lr | (chip == 3))
    def _():
        for j in range(parts):
            for e in range(2):
                fwd_lr(e, j).wait_send()

    @pl.when(passes_on)
    def _():
        for j in range(parts):
            for e in range(2):
                fwd_lr_on(e, j).wait_send()
    meta_copy(0, 1).wait_send()
    for offset, cols in OWNERS:
        @pl.when(owned_at(offset, cols) & exists(offset))
        def _(offset=offset):
            for e in range(2):
                meta_copy(offset, e).wait_send()
    for e in range(2):
        part_copy(OWN, e).wait_send()

    def drain(s, carry):
        @pl.when(uses(s))
        def _():
            for e in range(2):
                part_copy(s, e).wait_send()
                mirror_copy(s, e, offset_of(s)).wait_send()
        return carry

    lax.fori_loop(0, 4, drain, 0)


def per_device(genotypes, positions):
    devices = lax.axis_size("snp")
    rows, words = genotypes.shape
    parts = words // (2 * LANES)
    piece = (rows, LANES)
    dma = pltpu.SemaphoreType.DMA
    return pl.pallas_call(
        functools.partial(kernel, devices),
        out_shape=pltpu.VMEM((rows, (2 * REACH + 1) * LANES), jnp.float32),
        in_specs=[pl.BlockSpec(memory_space=pltpu.HBM)] * 2,
        out_specs=pl.BlockSpec(memory_space=pltpu.VMEM),
        scratch_shapes=[
            pltpu.VMEM((1, rows), jnp.int32),
            pltpu.VMEM((5, 2, parts) + piece, jnp.int32),
            pltpu.VMEM((parts,) + piece, jnp.int32),
            pltpu.VMEM((parts, CODES * LANES, 2 * rows), jnp.bfloat16),
            pltpu.VMEM((2 * rows, CODES * LANES), jnp.bfloat16),
            pltpu.VMEM((5, 2, 2) + piece, jnp.float32),
            pltpu.VMEM((5, 2) + piece, jnp.float32),
            pltpu.VMEM((5, 2, 3) + piece, jnp.bfloat16),
            pltpu.VMEM((5, 2) + piece, jnp.int32),
            pltpu.VMEM((2, 3, GROUP, LANES), jnp.bfloat16),
            pltpu.VMEM((8, LANES), jnp.int32),
            pltpu.VMEM((7, 2, 8, LANES), jnp.int32),
            pltpu.VMEM((4, 2) + piece, jnp.bfloat16),
            pltpu.VMEM((7, 2) + piece, jnp.bfloat16),
            pltpu.VMEM((8, LANES), jnp.float32),
            pltpu.SemaphoreType.REGULAR,
            dma((2, parts)),
            dma,
            dma((2, 2, parts)),
            dma((2, 2, parts)),
            dma((2, parts)),
            dma((5, 2, parts)),
            dma((7, 2)),
            dma((7, 2)),
            dma((parts,)),
            dma((5, 2)),
            dma((5, 2)),
            dma((4, 2)),
            dma((7, 2)),
        ],
        compiler_params=pltpu.CompilerParams(
            collective_id=0, has_side_effects=True, vmem_limit_bytes=60 * 1024 * 1024
        ),
    )(genotypes, positions.reshape(1, rows))


def solution(mesh):
    return jax.shard_map(
        per_device,
        mesh=mesh,
        in_specs=(P(("arm", "snp"), None), P(("arm", "snp"))),
        out_specs=P(("arm", "snp"), None),
        check_vma=False,
    )
```

```python
import functools

import jax
import jax.numpy as jnp
from jax import lax
from jax.experimental import pallas as pl
from jax.experimental.pallas import tpu as pltpu
from jax.sharding import PartitionSpec as P

REACH = 6
BAND_BP = 1000000
COLS = 4
LANES = 128
CODES = 16
RL, LR, ZRL, ZLR, OWN = range(5)
MESH = pl.DeviceIdType.MESH
I16 = jnp.int16
GROUP = 16
OWNERS = ((1, (0, 3)), (2, (0, 1)), (3, (2, 3)), (-2, (0, 1)), (-1, (2, 3)), (-3, (0, 3)))


def any_of(col, cols):
    hit = col == cols[0]
    for c in cols[1:]:
        hit = hit | (col == c)
    return hit


def lookup(half, bit, v0, v1, v2, zero):
    high = 2 << bit
    low_set = (half & I16(1 << bit)) != I16(0)
    high_set = (half & I16(high if high < 32768 else -32768)) != I16(0)
    return jnp.where(high_set, jnp.where(low_set, zero, v2), jnp.where(low_set, v1, v0))


def values_of(missing, dosage, samples):
    tally = samples - missing.astype(jnp.float32)
    allele = (dosage.astype(jnp.float32) + 1.0) / (2.0 * tally + 2.0)
    spread = lax.rsqrt(2.0 * allele * (1.0 - allele))
    return [(code - 2.0 * allele) * spread for code in (0.0, 1.0, 2.0)]


def kernel(devices, geno, pos_hbm, out, pos, buf, xbuf, own_t, panel, acc, part, tab, place_of,
           lane_tab, meta_out, meta_in, mir_out, mir_in,
           lane_val, late_sem, load_sem, pos_sem, x_send, fwd_send, fwd2_send, arrive, meta_send, meta_recv, sib_send,
           part_send, part_recv, mir_send, mir_recv):
    rows = pos_hbm.shape[1]
    words = geno.shape[1]
    parts = words // (2 * LANES)
    samples = float(words * CODES)
    me = lax.axis_index("snp")
    chips = devices // 2
    core = lax.rem(me, 2)
    chip = me // 2
    col = lax.rem(chip, COLS)
    base = chip - col

    def exists(offset):
        return (chip + offset >= 0) & (chip + offset < chips)

    def owned_at(offset, cols):
        there = any_of(col, cols)
        if offset == 1:
            return there & (chip > 0)
        return there | (chip == 1) if offset == -1 else there

    left = base + lax.rem(col + COLS - 1, COLS)
    right = base + lax.rem(col + 1, COLS)
    sibling = me + 1 - 2 * core

    def core_of(c, k):
        return {"snp": c * 2 + k}

    barrier = pltpu.get_barrier_semaphore()

    first = me == 0

    def greet(c):
        @pl.when(~first)
        def _():
            for k in range(2):
                pl.semaphore_signal(barrier, inc=1, device_id=core_of(c, k), device_id_type=MESH)

    def greets(c):
        return 2 - ((c == 0) & ~first).astype(jnp.int32)

    @pl.when(~first)
    def _():
        pl.semaphore_signal(barrier, inc=1, device_id={"snp": sibling}, device_id_type=MESH)
    greet(left)
    greet(right)
    greeted = greets(left) + greets(right) + (me != 1).astype(jnp.int32)
    for offset in (COLS, -COLS, 1, -1, 2, -2, 3, -3):
        @pl.when(exists(offset))
        def _(offset=offset):
            greet(chip + offset)
        greeted = greeted + greets(chip + offset) * exists(offset).astype(jnp.int32)

    loads = []
    for e in range(2):
        half = core if e == 0 else 1 - core
        for j in range(parts):
            lane = pl.multiple_of((half * parts + j) * LANES, LANES)
            dst = buf.at[OWN, 0, j] if e == 0 else xbuf.at[j]
            loads.append(pltpu.make_async_copy(geno.at[:, pl.ds(lane, LANES)], dst, load_sem.at[e, j]))
            loads[-1].start()

    pos_load = pltpu.make_async_copy(pos_hbm, pos, pos_sem)
    pos_load.start()

    def own_piece(e, j):
        return buf.at[OWN, 0, j] if e == 0 else xbuf.at[j]


    sends_left = col >= 1
    sends_right = (col == 0) | (col == 3)
    uses_rl = (col >= 1) | (chip == 0)
    uses_lr = (col <= 2) & (chip != 1)
    top = chip < COLS

    def lag_of(s):
        late = jnp.where(top, parts + 1, jnp.where(col == 2, 1, 0))
        return jnp.where(s == RL, jnp.where(chip == 0, parts + 1, 0), jnp.where(s == LR, late, jnp.where((s == ZLR) & (col == 2), 2, 1)))

    lag = lag_of(LR)
    steps = parts + 1 + jnp.where(top, parts + 1, jnp.where(col == 2, 2, 1))
    late_end = (chip == 1) | (chip == 3)
    dz_rl = jnp.where(col == 3, -1, 1)
    dz_lr = jnp.where(col == 0, 1, -1)
    off_rl = jnp.where(col == 3, -2, 1)
    off_lr = jnp.where(col == 0, 3, jnp.where(col == 1, -1, -2))
    off_zrl = off_rl - COLS * dz_rl
    off_zlr = off_lr - COLS * dz_lr

    def offset_of(s):
        return jnp.where(s == RL, off_rl, jnp.where(s == LR, off_lr, jnp.where(s == ZRL, off_zrl, off_zlr)))

    z_rl = exists(-COLS * dz_rl)
    z_lr = exists(-COLS * dz_lr)

    def uses(s):
        z = jnp.where(s == ZRL, z_rl & (col >= 1), z_lr & (col <= 2))
        return jnp.where(s == RL, uses_rl, jnp.where(s == LR, uses_lr, z))

    for copy in loads:
        copy.wait()
    pos_load.wait()
    missing = jnp.zeros((rows, LANES), jnp.int32)
    dosage = jnp.zeros((rows, LANES), jnp.int32)
    for e in range(2):
        for j in range(parts):
            word = own_piece(e, j)[...]
            low = word & 0x55555555
            high = lax.shift_right_logical(word, 1) & 0x55555555
            gone = lax.population_count(low & high)
            missing = missing + gone
            dosage = dosage + lax.population_count(low) + 2 * lax.population_count(high) - 3 * gone
    counts = []
    for x in (missing, dosage):
        total = jnp.broadcast_to(jnp.sum(x, axis=1, keepdims=True), (rows, LANES))
        counts.append(total.T[0:1])
    meta_out[0:1] = pos[...]
    meta_out[1:2] = counts[0]
    meta_out[2:3] = counts[1]
    meta_out[3:8] = jnp.zeros((5, LANES), jnp.int32)

    def meta_copy(offset, e):
        k = core if e == 0 else 1 - core
        return pltpu.make_async_remote_copy(
            src_ref=meta_out, dst_ref=meta_in.at[3 - offset, e], send_sem=meta_send.at[3 + offset, e],
            recv_sem=meta_recv.at[3 - offset, e],
            device_id={"snp": sibling} if offset == 0 else core_of(chip + offset, k), device_id_type=MESH)

    def hop(src, send_sem, s, e, j, target):
        return pltpu.make_async_remote_copy(
            src_ref=src, dst_ref=buf.at[s, e, j], send_sem=send_sem, recv_sem=arrive.at[s, e, j],
            device_id=target, device_id_type=MESH)

    def x_hop(e, j, way):
        c = jnp.where(col == 1, base + 3, left) if way == RL else jnp.where(chip == 0, 2, right)
        return hop(own_piece(e, j), x_send.at[way, e, j], way, e, j, core_of(c, core if e == 0 else 1 - core))

    def x_hop_down(e, j):
        return hop(own_piece(e, j), fwd_send.at[LR, e, j], ZLR, e, j,
                   core_of(chip + 1, core if e == 0 else 1 - core))

    def to_first(e, way):
        return (chip == 3) & (core == e) if way == LR else False

    def x_hop_first(e, j):
        return hop(own_piece(e, j), x_send.at[LR, e, j], RL, e, j, core_of(0, core if e == 0 else 1 - core))

    def to_sibling(j):
        return hop(xbuf.at[j], sib_send.at[j], OWN, 1, j, {"snp": sibling})

    def greet_sibling():
        meta_copy(0, 1).start()
        for j in range(parts):
            to_sibling(j).start()

    def send_first():
        for offset, cols in OWNERS:
            waits = chip + offset == 0 if offset in (-1, -3) else False

            @pl.when(owned_at(offset, cols) & exists(offset) & ~jnp.bool_(waits))
            def _(offset=offset):
                for e in range(2):
                    meta_copy(offset, e).start()

        @pl.when(me != 1)
        def _():
            greet_sibling()

        for way, sends in ((RL, sends_left), (LR, sends_right)):
            for j in range(parts):
                for e in range(2):
                    @pl.when(sends & ~jnp.bool_(to_first(e, way)))
                    def _(way=way, e=e, j=j):
                        x_hop(e, j, way).start()

        @pl.when(chip == 3)
        def _():
            for j in range(parts):
                for e in range(2):
                    x_hop_down(e, j).start()

        for e in range(2):
            @pl.when((chip == 1) & (core != e))
            def _(e=e):
                for j in range(parts):
                    x_hop_first(e, j).start()

    @pl.when(first)
    def _():
        pl.semaphore_wait(barrier, greeted)
        pl.semaphore_signal(late_sem, inc=1, device_id={"snp": sibling}, device_id_type=MESH)
        for c in range(1, COLS):
            for k in range(2):
                pl.semaphore_signal(late_sem, inc=1, device_id=core_of(c, k), device_id_type=MESH)
        send_first()

    def fill_tables(s, e, counts8):
        place_of[s, e] = jnp.broadcast_to(counts8.T[:, 0:1], (rows, LANES))
        for i, v in enumerate(values_of(counts8[1:2], counts8[2:3], samples)):
            lane_val[i:i + 1] = v
        columns = lane_val[...].T
        for i in range(3):
            tab[s, e, i] = jnp.broadcast_to(columns[:, i:i + 1], (rows, LANES)).astype(jnp.bfloat16)

    def lanes_of(e, counts8):
        for i, v in enumerate(values_of(counts8[1:2], counts8[2:3], samples)):
            lane_tab[e, i] = jnp.broadcast_to(v, (GROUP, LANES)).astype(jnp.bfloat16)

    def halves_of(word):
        return word.astype(I16), lax.shift_right_logical(word, 16).astype(I16)

    def turn(e, j):
        turned = buf[OWN, e, j].T
        v0, v1, v2 = (lane_tab[e, i] for i in range(3))
        zero = jnp.zeros_like(v0)
        for g in range(0, LANES, GROUP):
            halves = halves_of(turned[g:g + GROUP])
            for q in range(CODES):
                own_t[j, q * LANES + g:q * LANES + g + GROUP, e * rows:(e + 1) * rows] = lookup(
                    halves[q // 8], 2 * (q % 8), v0, v1, v2, zero)

    lane_val[...] = jnp.zeros_like(lane_val)
    acc[...] = jnp.zeros_like(acc)
    fill_tables(OWN, 0, meta_out[...])
    lanes_of(0, meta_out[...])

    def turn_own(j, carry):
        turn(0, j)
        return carry

    lax.fori_loop(0, parts, turn_own, 0)
    @pl.when(~first)
    def _():
        pl.semaphore_wait(barrier, greeted)
        send_first()

    out[...] = jnp.zeros_like(out)

    def batch(s, j):
        for e in range(2):
            for g in range(0, rows, GROUP):
                halves = halves_of(buf[s, e, j, g:g + GROUP])
                v0, v1, v2 = (tab[s, e, i, g:g + GROUP] for i in range(3))
                zero = jnp.zeros_like(v0)
                for q in range(CODES):
                    panel[e * rows + g:e * rows + g + GROUP, q * LANES:(q + 1) * LANES] = lookup(
                        halves[q // 8], 2 * (q % 8), v0, v1, v2, zero)
        product = lax.dot_general(panel[...], own_t[j], (((1,), (0,)), ((), ())),
                                  preferred_element_type=jnp.float32)
        for e in range(2):
            for c in range(2):
                tile = product[e * rows:(e + 1) * rows, c * LANES:(c + 1) * LANES]
                acc[s, e, c] += tile

    def meta_arrived(slot, e):
        pltpu.make_async_remote_copy(
            src_ref=meta_out, dst_ref=meta_in.at[slot, e], send_sem=meta_send.at[slot, e],
            recv_sem=meta_recv.at[slot, e], device_id={"snp": sibling}, device_id_type=MESH).wait_recv()

    @pl.when(me == 1)
    def _():
        pl.semaphore_wait(late_sem, 1)
        greet_sibling()

    meta_arrived(3, 1)
    fill_tables(OWN, 1, meta_in[3, 1])
    lanes_of(1, meta_in[3, 1])

    def part_copy(s, e):
        return pltpu.make_async_remote_copy(
            src_ref=acc.at[s, e, 1], dst_ref=part.at[s, 1 - e], send_sem=part_send.at[s, e],
            recv_sem=part_recv.at[s, 1 - e], device_id={"snp": sibling}, device_id_type=MESH)

    def part_arrived(s, e):
        pltpu.make_async_remote_copy(
            src_ref=acc.at[s, e, 1], dst_ref=part.at[s, e], send_sem=part_send.at[s, e],
            recv_sem=part_recv.at[s, e], device_id={"snp": sibling}, device_id_type=MESH).wait_recv()

    def own_step(j):
        to_sibling(j).wait_recv()
        turn(1, j)
        batch(OWN, j)

        @pl.when(j == parts - 1)
        def _():
            for e in range(2):
                part_copy(OWN, e).start()

    passes_rl = (col >= 1) & exists(COLS * dz_rl)
    passes_lr = uses_lr & exists(COLS * dz_lr) & (chip > 0)
    passes_on = (col == 1) & (chip != 1)

    def fwd_rl(e, j):
        return hop(buf.at[RL, e, j], fwd_send.at[RL, e, j], ZRL, e, j, core_of(chip + COLS * dz_rl, core))

    def fwd_lr(e, j):
        return hop(buf.at[LR, e, j], fwd_send.at[LR, e, j], ZLR, e, j, core_of(chip + COLS * dz_lr, core))

    def fwd_lr_on(e, j):
        return hop(buf.at[LR, e, j], fwd2_send.at[e, j], LR, e, j, core_of(right, core))

    def arrived(s, e, j):
        hop(buf.at[s, e, j], fwd_send.at[RL, e, j], s, e, j, {"snp": sibling}).wait_recv()

    def put(tile, at):
        @pl.when((at >= 0) & (at <= 2 * REACH))
        def _():
            out[:, pl.ds(pl.multiple_of(at * LANES, LANES), LANES)] = tile

    def finished(s, e):
        part_arrived(s, e)
        tile = (acc[s, e, 0] + part[s, e]) / samples
        near = jnp.abs(place_of[s, e] - pos[...]) <= BAND_BP
        return jnp.where(near, tile, jnp.zeros_like(tile))

    def mirror_copy(s, e, offset):
        k = core if e == 0 else 1 - core
        return pltpu.make_async_remote_copy(
            src_ref=mir_out.at[s, e], dst_ref=mir_in.at[3 - offset, e], send_sem=mir_send.at[s, e],
            recv_sem=mir_recv.at[3 - offset, e], device_id=core_of(chip + offset, k), device_id_type=MESH)

    def column_of(offset, e):
        k = core if e == 0 else 1 - core
        return 2 * (offset + 3) + k - core

    def finish(s):
        offset = offset_of(s)
        for e in range(2):
            tile = finished(s, e)
            mir_out[s, e] = tile.astype(jnp.bfloat16)
            mirror_copy(s, e, offset).start()
            put(tile.T, column_of(offset, e))

    def step(t, carry):
        @pl.when(top & (col >= 1) & (t == parts))
        def _():
            pl.semaphore_wait(late_sem, 1)

            for offset in (-1, -3):
                @pl.when(late_end & (chip + offset == 0))
                def _(offset=offset):
                    for e in range(2):
                        meta_copy(offset, e).start()
            for e in range(2):
                @pl.when((chip == 1) & (core == e))
                def _(e=e):
                    for j in range(parts):
                        x_hop_first(e, j).start()

                @pl.when((chip == 3) & (core == e))
                def _(e=e):
                    for j in range(parts):
                        x_hop(e, j, LR).start()

        behind = t - lag
        for e in range(2):
            at_rl = t - lag_of(RL)

            @pl.when((at_rl >= 0) & (at_rl < parts) & uses_rl)
            def _(e=e, at_rl=at_rl):
                arrived(RL, e, at_rl)

                @pl.when(passes_rl)
                def _():
                    fwd_rl(e, at_rl).start()

            @pl.when((behind >= 0) & (behind < parts) & uses_lr)
            def _(e=e):
                arrived(LR, e, behind)

                @pl.when(passes_on)
                def _():
                    fwd_lr_on(e, behind).start()

                @pl.when(passes_lr)
                def _():
                    fwd_lr(e, behind).start()

        @pl.when(t < parts - 1)
        def _():
            own_step(t + 1)

        @pl.when(t == parts)
        def _():
            for e in range(2):
                put(finished(OWN, e).T, column_of(0, e))

        def stream(s, inner):
            j = t - lag_of(s)

            @pl.when(uses(s) & (j >= 0) & (j < parts))
            def _():
                @pl.when(j == 0)
                def _():
                    slot = offset_of(s) + 3
                    for e in range(2):
                        meta_arrived(slot, e)
                        fill_tables(s, e, meta_in[slot, e])

                @pl.when(s >= ZRL)
                def _():
                    for e in range(2):
                        arrived(s, e, j)
                batch(s, j)

                @pl.when(j == parts - 1)
                def _():
                    for e in range(2):
                        part_copy(s, e).start()

            @pl.when(uses(s) & (j == parts))
            def _():
                finish(s)
            return inner

        lax.fori_loop(RL, OWN, stream, 0)
        return carry

    lax.fori_loop(-1, steps, step, 0)

    for way, sends in ((RL, sends_left), (LR, sends_right | (chip == 1))):
        @pl.when(sends)
        def _(way=way):
            for j in range(parts):
                for e in range(2):
                    x_hop(e, j, way).wait_send()
    for j in range(parts):
        to_sibling(j).wait_send()

    @pl.when(passes_rl)
    def _():
        for j in range(parts):
            for e in range(2):
                fwd_rl(e, j).wait_send()

    @pl.when(passes_lr | (chip == 3))
    def _():
        for j in range(parts):
            for e in range(2):
                fwd_lr(e, j).wait_send()

    @pl.when(passes_on)
    def _():
        for j in range(parts):
            for e in range(2):
                fwd_lr_on(e, j).wait_send()
    meta_copy(0, 1).wait_send()
    for offset, cols in OWNERS:
        @pl.when(owned_at(offset, cols) & exists(offset))
        def _(offset=offset):
            for e in range(2):
                meta_copy(offset, e).wait_send()
    for e in range(2):
        part_copy(OWN, e).wait_send()

    def drain(s, carry):
        @pl.when(uses(s))
        def _():
            for e in range(2):
                part_copy(s, e).wait_send()
                mirror_copy(s, e, offset_of(s)).wait_send()
        return carry

    lax.fori_loop(0, 4, drain, 0)

    for offset, cols in OWNERS:
        @pl.when(owned_at(offset, cols) & exists(offset))
        def _(offset=offset):
            for e in range(2):
                pltpu.make_async_remote_copy(
                    src_ref=mir_out.at[0, e], dst_ref=mir_in.at[3 + offset, e], send_sem=mir_send.at[0, e],
                    recv_sem=mir_recv.at[3 + offset, e], device_id={"snp": sibling},
                    device_id_type=MESH).wait_recv()
                put(mir_in[3 + offset, e].astype(jnp.float32), column_of(offset, e))


def per_device(genotypes, positions):
    devices = lax.axis_size("snp")
    rows, words = genotypes.shape
    parts = words // (2 * LANES)
    piece = (rows, LANES)
    dma = pltpu.SemaphoreType.DMA
    return pl.pallas_call(
        functools.partial(kernel, devices),
        out_shape=pltpu.VMEM((rows, (2 * REACH + 1) * LANES), jnp.float32),
        in_specs=[pl.BlockSpec(memory_space=pltpu.HBM)] * 2,
        out_specs=pl.BlockSpec(memory_space=pltpu.VMEM),
        scratch_shapes=[
            pltpu.VMEM((1, rows), jnp.int32),
            pltpu.VMEM((5, 2, parts) + piece, jnp.int32),
            pltpu.VMEM((parts,) + piece, jnp.int32),
            pltpu.VMEM((parts, CODES * LANES, 2 * rows), jnp.bfloat16),
            pltpu.VMEM((2 * rows, CODES * LANES), jnp.bfloat16),
            pltpu.VMEM((5, 2, 2) + piece, jnp.float32),
            pltpu.VMEM((5, 2) + piece, jnp.float32),
            pltpu.VMEM((5, 2, 3) + piece, jnp.bfloat16),
            pltpu.VMEM((5, 2) + piece, jnp.int32),
            pltpu.VMEM((2, 3, GROUP, LANES), jnp.bfloat16),
            pltpu.VMEM((8, LANES), jnp.int32),
            pltpu.VMEM((7, 2, 8, LANES), jnp.int32),
            pltpu.VMEM((4, 2) + piece, jnp.bfloat16),
            pltpu.VMEM((7, 2) + piece, jnp.bfloat16),
            pltpu.VMEM((8, LANES), jnp.float32),
            pltpu.SemaphoreType.REGULAR,
            dma((2, parts)),
            dma,
            dma((2, 2, parts)),
            dma((2, 2, parts)),
            dma((2, parts)),
            dma((5, 2, parts)),
            dma((7, 2)),
            dma((7, 2)),
            dma((parts,)),
            dma((5, 2)),
            dma((5, 2)),
            dma((4, 2)),
            dma((7, 2)),
        ],
        compiler_params=pltpu.CompilerParams(
            collective_id=0, has_side_effects=True, vmem_limit_bytes=60 * 1024 * 1024
        ),
    )(genotypes, positions.reshape(1, rows))


def solution(mesh):
    return jax.shard_map(
        per_device,
        mesh=mesh,
        in_specs=(P(("arm", "snp"), None), P(("arm", "snp"))),
        out_specs=P(("arm", "snp"), None),
        check_vma=False,
    )
```
